32 devices in a mesh: dp: 8 (over y, x, core), enc: 4 (over z).
Axes of the slice: x: 2, y: 2, z: 4, core: 2. Of those that a mesh axis runs over, the one named last changes fastest.
Arguments:
- patches: bfloat16 [4096, 1280], P(('dp', 'enc')), may hold values from -6 to 6
- cotangent: bfloat16 [4096, 1280], P(('dp', 'enc')), may hold values from -6 to 6
- counts: int32 [8, 4, 8, 4], replicated, may hold values from 0 to 8, as said below
- gain: float32 [1280], replicated, may hold values from 0.25 to 1.75
- w_qkv: bfloat16 [1280, 3840], replicated, may hold values from -0.15625 to 0.15625
- w_out: bfloat16 [1280, 1280], replicated, may hold values from -0.15625 to 0.15625
Outputs:
- output: bfloat16 [4096, 1280], P(('dp', 'enc'))
- grad_patches: bfloat16 [4096, 1280], P(('dp', 'enc'))
The draws below stay inside these ranges and needn't reach their ends.
Inputs may be any that keep to these rules, and one draw needn't show every extreme that they name: For every sending device the counts to all destinations sum to 128; each count is at most 8; some destination device receives 8 rows from every sender, and every sender fills its 8 slots to some destination.
All inputs are finite; a program needn't handle non-finite values.
Results may differ from the reference program's by a relative error of at most 0.0039.
Values may be sent and summed in bfloat16 or wider, within the bound.
No kernel may reach another device: no remote copies, remote signals or barrier semaphores. Data moves between devices by JAX's collectives and lax.ppermute only.
A program may use at most 128 MiB of HBM per device.

```python
import jax
import jax.numpy as jnp
from jax import lax

D = 1280
H = 16
HD = 80
HOME = 128
CAP = 8
ROWS = 4096
N_DP = 8
N_ENC = 4


def draw_counts(key, part):
    devices = N_DP * N_ENC
    slot_total = devices * CAP
    key_one, key_two, key_three = jax.random.split(key, 3)
    favored = jax.random.randint(key_one, (), 0, devices)
    weighting = jax.random.randint(key_two, (devices,), 0, 3)
    senders = jax.random.split(key_three, devices)
    shuffled = jax.vmap(lambda sub: jax.random.permutation(sub, slot_total))(senders)
    target = jnp.arange(slot_total, dtype=jnp.int32) // CAP
    score = shuffled + (weighting[target] + 4 * (target == favored).astype(jnp.int32)) * slot_total
    ordering = jnp.argsort(-score, axis=1, stable=True)
    placed = jnp.argsort(ordering, axis=1, stable=True)
    chosen = (placed < HOME).astype(jnp.int32)
    tally = chosen.reshape(devices, devices, CAP).sum(axis=-1).astype(jnp.int32)
    return tally.reshape(N_DP, N_ENC, N_DP, N_ENC)


def block_scale(own_key, dims, shards, least, top_value):
    def one(position, blocks):
        steps = jax.random.uniform(jax.random.fold_in(jax.random.fold_in(own_key, 6), position), (blocks,), jnp.float32, least / len(shards), top_value / len(shards))
        return jnp.repeat(jnp.exp(steps), dims[position] // blocks).reshape((-1,) + (1,) * (len(dims) - position - 1))

    loudness = one(*shards[0])
    for cut in shards[1:]:
        loudness = loudness * one(*cut)
    return loudness


def noise(rng, shape, spread, most, shards=(), held_as=jnp.bfloat16):
    level = block_scale(rng, shape, shards, -0.22, 0.18) if shards else 1.0
    drawn = jax.random.normal(rng, shape, jnp.float32) * spread * level
    return jnp.minimum(jnp.maximum(drawn, -most), most).astype(held_as)


def setup_inputs(seed: int = 0) -> dict:
    key_list = jax.random.split(jax.random.key(seed), 7)
    patches = noise(key_list[0], (ROWS, D), 1.0, 6.0, ((0, 32),))
    cotangent = noise(key_list[1], (ROWS, D), 1.0, 6.0, ((0, 32),))
    counts = draw_counts(jax.random.fold_in(key_list[6], 71), 0)
    gain = jnp.clip(1.0 + 0.15 * jax.random.normal(key_list[3], (D,), jnp.float32), 0.25, 1.75)
    w_qkv = noise(key_list[4], (D, 3 * D), D ** -0.5, 0.15625)
    w_out = noise(key_list[5], (D, D), D ** -0.5, 0.15625)
    return {"patches": patches, "cotangent": cotangent, "counts": counts, "gain": gain, "w_qkv": w_qkv, "w_out": w_out}


eps = 1e-06

def image_layer(x, dy, valid, gain, w_qkv, w_out):
    inv_scale = HD ** (-0.5)
    xf = x.astype(jnp.float32)
    inv = lax.rsqrt(lax.optimization_barrier(jnp.mean(xf * xf, axis=-1, keepdims=True)) + eps)
    normed = (xf * inv * gain).astype(jnp.bfloat16)
    proj = jnp.einsum('imd,de->ime', normed.astype(jnp.float32), w_qkv.astype(jnp.float32))
    proj = proj.astype(jnp.bfloat16)
    images, length = (x.shape[0], x.shape[1])
    proj = proj.reshape(images, length, 3, H, HD)
    query = proj[:, :, 0].astype(jnp.float32)
    keys = proj[:, :, 1].astype(jnp.float32)
    values = proj[:, :, 2].astype(jnp.float32)
    scores = jnp.einsum('iqhd,ikhd->ihqk', query, keys) * inv_scale
    scores = jnp.where(valid[:, None, None, :], scores, -1000000000.0)
    attn = jax.nn.softmax(scores, axis=-1)
    attn_b = attn.astype(jnp.bfloat16)
    context = jnp.einsum('ihqk,ikhd->iqhd', attn_b.astype(jnp.float32), values).astype(jnp.bfloat16)
    context = context.reshape(images, length, D)
    out_f = jnp.einsum('imd,de->ime', context.astype(jnp.float32), w_out.astype(jnp.float32))
    output = (xf + out_f).astype(jnp.bfloat16)
    d_context = jnp.einsum('ime,de->imd', dy.astype(jnp.float32), w_out.astype(jnp.float32)).astype(jnp.bfloat16)
    d_ctx4 = d_context.reshape(images, length, H, HD).astype(jnp.float32)
    d_attn = jnp.einsum('iqhd,ikhd->ihqk', d_ctx4, values)
    d_scores = attn * (d_attn - lax.optimization_barrier(jnp.sum(attn * d_attn, axis=-1, keepdims=True)))
    d_scores_b = d_scores.astype(jnp.bfloat16).astype(jnp.float32)
    d_query = jnp.einsum('ihqk,ikhd->iqhd', d_scores_b, keys) * inv_scale
    d_key = jnp.einsum('ihqk,iqhd->ikhd', d_scores_b, query) * inv_scale
    d_value = jnp.einsum('ihqk,iqhd->ikhd', attn_b.astype(jnp.float32), d_ctx4)
    d_all = jnp.concatenate([d_query.reshape(images, length, D), d_key.reshape(images, length, D), d_value.reshape(images, length, D)], axis=-1)
    d_proj = d_all.astype(jnp.bfloat16)
    d_normed = jnp.einsum('ime,de->imd', d_proj.astype(jnp.float32), w_qkv.astype(jnp.float32))
    scaled = gain * d_normed
    grad = dy.astype(jnp.float32) + inv * scaled - xf * inv ** 3 * lax.optimization_barrier(jnp.mean(xf * scaled, axis=-1, keepdims=True))
    return (output, grad.astype(jnp.bfloat16))

def reference(patches, cotangent, counts, gain, w_qkv, w_out):
    devices = N_DP * N_ENC
    plan = counts.reshape(devices, devices).astype(jnp.int32)
    offsets = jnp.cumsum(plan, axis=1).astype(jnp.int32) - plan
    slots = jnp.arange(CAP, dtype=jnp.int32)
    index = offsets[:, :, None] + slots[None, None, :]
    valid = slots[None, None, :] < plan[:, :, None]
    safe = jnp.clip(index, 0, HOME - 1).astype(jnp.int32)
    source = jnp.arange(devices, dtype=jnp.int32)[:, None, None]
    home_x = patches.reshape(devices, HOME, D)
    home_dy = cotangent.reshape(devices, HOME, D)
    sent_x = jnp.where(valid[..., None], home_x[source, safe], 0).astype(jnp.bfloat16)
    sent_dy = jnp.where(valid[..., None], home_dy[source, safe], 0).astype(jnp.bfloat16)
    length = N_ENC * devices * CAP

    def regroup(array):
        shaped = array.reshape(N_DP, N_ENC, N_DP, N_ENC, CAP, -1)
        return shaped.transpose(2, 3, 0, 1, 4, 5).reshape(N_DP, length, -1)
    group_x = regroup(sent_x)
    group_dy = regroup(sent_dy)
    group_valid = regroup(valid[..., None])[..., 0]

    def per_group(operands):
        out_one, grad_one = image_layer(operands[0][None], operands[1][None], operands[2][None], gain, w_qkv, w_out)
        return (out_one[0], grad_one[0])
    outputs, grads = lax.map(per_group, (group_x, group_dy, group_valid))

    def ungroup(array):
        shaped = array.reshape(N_DP, N_ENC, N_DP, N_ENC, CAP, D)
        return shaped.transpose(2, 3, 0, 1, 4, 5).reshape(devices, devices, CAP, D)
    target = jnp.where(valid, source * HOME + index, devices * HOME).reshape(-1).astype(jnp.int32)
    output = jnp.zeros((devices * HOME, D), jnp.bfloat16).at[target].set(ungroup(outputs).reshape(-1, D), mode='drop')
    grad_patches = jnp.zeros((devices * HOME, D), jnp.bfloat16).at[target].set(ungroup(grads).reshape(-1, D), mode='drop')
    return (output, grad_patches)
```

```python
import functools

import jax
import jax.numpy as jnp
from jax import lax
from jax.experimental import pallas as pl
from jax.experimental.pallas import tpu as pltpu
from jax.sharding import Mesh
from jax.sharding import PartitionSpec as P

H = 16
HD = 80
LANES = 128
eps = 1e-06
LOG2E = 1.4426950408889634
DEAD = -1000000000.0
VMEM_LIMIT = 56 * 1024 * 1024


def nt_dot(a, b):
    return lax.dot_general(a, b, (((1,), (1,)), ((), ())), preferred_element_type=jnp.float32)


def nn_dot(a, b):
    return lax.dot_general(a, b, (((1,), (0,)), ((), ())), preferred_element_type=jnp.float32)


def column_step(total):
    for step in (640, 512, 384, 256, 128):
        if total % step == 0:
            return step
    return total


def params(*semantics):
    return pltpu.CompilerParams(dimension_semantics=semantics, vmem_limit_bytes=VMEM_LIMIT)


def norm_project(x, gain, w_qkv):
    rows, width = x.shape
    cols = w_qkv.shape[1]
    step = column_step(cols)

    def body(x_ref, gain_ref, w_ref, out_ref, normed_ref):
        @pl.when(pl.program_id(0) == 0)
        def _():
            xf = x_ref[...].astype(jnp.float32)
            inv = lax.rsqrt(jnp.mean(xf * xf, axis=-1, keepdims=True) + eps)
            normed_ref[...] = (xf * inv * gain_ref[...]).astype(jnp.bfloat16)

        out_ref[...] = nn_dot(normed_ref[...], w_ref[...]).astype(jnp.bfloat16)

    return pl.pallas_call(
        body,
        grid=(cols // step,),
        in_specs=[
            pl.BlockSpec((rows, width), lambda n: (0, 0)),
            pl.BlockSpec((1, width), lambda n: (0, 0)),
            pl.BlockSpec((width, step), lambda n: (0, n)),
        ],
        out_specs=pl.BlockSpec((rows, step), lambda n: (0, n)),
        out_shape=jax.ShapeDtypeStruct((rows, cols), jnp.bfloat16),
        scratch_shapes=[pltpu.VMEM((rows, width), jnp.bfloat16)],
        compiler_params=params("arbitrary"),
        cost_estimate=pl.CostEstimate(
            flops=2 * rows * width * cols, bytes_accessed=2 * width * cols, transcendentals=0
        ),
        name="norm_project",
    )(x, gain, w_qkv)


def back_project(dy, w_out):
    rows, width = dy.shape
    step = 256

    def body(dy_ref, w_ref, out_ref):
        out_ref[...] = nt_dot(dy_ref[...], w_ref[...]).astype(jnp.bfloat16)

    return pl.pallas_call(
        body,
        grid=(width // step,),
        in_specs=[
            pl.BlockSpec((rows, width), lambda n: (0, 0)),
            pl.BlockSpec((step, width), lambda n: (n, 0)),
        ],
        out_specs=pl.BlockSpec((rows, step), lambda n: (0, n)),
        out_shape=jax.ShapeDtypeStruct((rows, width), jnp.bfloat16),
        compiler_params=params("arbitrary"),
        cost_estimate=pl.CostEstimate(
            flops=2 * rows * width * width, bytes_accessed=2 * width * width, transcendentals=0
        ),
        name="back_project",
    )(dy, w_out)


def head_window(head, width):
    tile = jnp.minimum(head * HD // LANES, width // LANES - 2)
    start = pl.multiple_of(tile * LANES, LANES)
    lane = lax.broadcasted_iota(jnp.int32, (1, 2 * LANES), 1) + start
    mask = jnp.logical_and(lane >= head * HD, lane < head * HD + HD)
    return start, mask


def query_side(qkv_blocks, d_context, key_bias):
    rows, width = d_context.shape
    blocks = len(qkv_blocks)
    scale = HD ** (-0.5)

    def body(*refs):
        qkv = refs[:blocks]
        dctx_ref, bias_ref, ctx_ref, dq_ref, stats_ref, stat_scratch = refs[blocks:]
        lane = lax.broadcasted_iota(jnp.int32, (1, LANES), 1)

        def head_step(head, _):
            start, mask = head_window(head, width)
            win = pl.ds(start, 2 * LANES)
            key_win = pl.ds(pl.multiple_of(start + width, LANES), 2 * LANES)
            value_win = pl.ds(pl.multiple_of(start + 2 * width, LANES), 2 * LANES)
            zero = jnp.zeros((), jnp.bfloat16)
            q = jnp.where(mask, qkv[0][:, win], zero)
            dc = jnp.where(mask, dctx_ref[:, win], zero)
            scores = [
                nt_dot(q, qkv[b][:, key_win]) * (scale * LOG2E)
                + bias_ref[:, b * rows : (b + 1) * rows]
                for b in range(blocks)
            ]
            top = functools.reduce(jnp.maximum, scores)
            top = jnp.max(top, axis=-1, keepdims=True)
            weights = [jnp.exp2(s - top) for s in scores]
            total = jnp.sum(functools.reduce(jnp.add, weights), axis=-1, keepdims=True)
            inv_total = 1.0 / total
            attn = [w * inv_total for w in weights]
            ctx = functools.reduce(
                jnp.add,
                [nn_dot(attn[b].astype(jnp.bfloat16), qkv[b][:, value_win]) for b in range(blocks)],
            )
            ctx_ref[:, win] = jnp.where(mask, ctx.astype(jnp.bfloat16), ctx_ref[:, win])
            d_attn = [nt_dot(dc, qkv[b][:, value_win]) for b in range(blocks)]
            inner = jnp.sum(
                functools.reduce(jnp.add, [attn[b] * d_attn[b] for b in range(blocks)]),
                axis=-1,
                keepdims=True,
            )
            d_scores = [(attn[b] * (d_attn[b] - inner)).astype(jnp.bfloat16) for b in range(blocks)]
            dq = functools.reduce(
                jnp.add, [nn_dot(d_scores[b], qkv[b][:, key_win]) for b in range(blocks)]
            )
            dq_ref[:, win] = jnp.where(mask, (dq * scale).astype(jnp.bfloat16), dq_ref[:, win])
            log_total = top + jnp.log2(total)
            stat = jnp.where(lane == head, log_total, stat_scratch[...])
            stat_scratch[...] = jnp.where(lane == head + H, inner, stat)
            return 0

        lax.fori_loop(0, H, head_step, 0)
        stats_ref[...] = jnp.transpose(stat_scratch[...])[: 2 * H]

    return pl.pallas_call(
        body,
        out_shape=(
            jax.ShapeDtypeStruct((rows, width), jnp.bfloat16),
            jax.ShapeDtypeStruct((rows, width), jnp.bfloat16),
            jax.ShapeDtypeStruct((2 * H, rows), jnp.float32),
        ),
        scratch_shapes=[pltpu.VMEM((rows, LANES), jnp.float32)],
        compiler_params=pltpu.CompilerParams(vmem_limit_bytes=VMEM_LIMIT),
        cost_estimate=pl.CostEstimate(
            flops=8 * H * rows * rows * blocks * 2 * LANES,
            bytes_accessed=6 * blocks * rows * width,
            transcendentals=0,
        ),
        name="query_side",
    )(*qkv_blocks, d_context, key_bias)


def key_side(qkv_blocks, dctx_blocks, stats_blocks, own_bias):
    rows, width = dctx_blocks[0].shape
    blocks = len(qkv_blocks)
    scale = HD ** (-0.5)

    def body(*refs):
        qkv = refs[:blocks]
        dctx = refs[blocks : 2 * blocks]
        stats = refs[2 * blocks : 3 * blocks]
        bias_ref, dk_ref, dv_ref = refs[3 * blocks :]

        def head_step(head, _):
            start, mask = head_window(head, width)
            win = pl.ds(start, 2 * LANES)
            key_win = pl.ds(pl.multiple_of(start + width, LANES), 2 * LANES)
            value_win = pl.ds(pl.multiple_of(start + 2 * width, LANES), 2 * LANES)
            zero = jnp.zeros((), jnp.bfloat16)
            k = jnp.where(mask, qkv[0][:, key_win], zero)
            v = jnp.where(mask, qkv[0][:, value_win], zero)
            dk = jnp.zeros((rows, 2 * LANES), jnp.float32)
            dv = jnp.zeros((rows, 2 * LANES), jnp.float32)
            for b in range(blocks):
                q = qkv[b][:, win]
                dc = dctx[b][:, win]
                log_total = stats[b][pl.ds(head, 1), :]
                inner = stats[b][pl.ds(head + H, 1), :]
                scores = nt_dot(k, q) * (scale * LOG2E) + bias_ref[...]
                attn = jnp.exp2(scores - log_total)
                dv = dv + nn_dot(attn.astype(jnp.bfloat16), dc)
                d_scores = attn * (nt_dot(v, dc) - inner)
                dk = dk + nn_dot(d_scores.astype(jnp.bfloat16), q)
            dk_ref[:, win] = jnp.where(mask, (dk * scale).astype(jnp.bfloat16), dk_ref[:, win])
            dv_ref[:, win] = jnp.where(mask, dv.astype(jnp.bfloat16), dv_ref[:, win])
            return 0

        lax.fori_loop(0, H, head_step, 0)

    return pl.pallas_call(
        body,
        out_shape=(
            jax.ShapeDtypeStruct((rows, width), jnp.bfloat16),
            jax.ShapeDtypeStruct((rows, width), jnp.bfloat16),
        ),
        compiler_params=pltpu.CompilerParams(vmem_limit_bytes=VMEM_LIMIT),
        cost_estimate=pl.CostEstimate(
            flops=8 * H * rows * rows * blocks * 2 * LANES,
            bytes_accessed=6 * blocks * rows * width,
            transcendentals=0,
        ),
        name="key_side",
    )(*qkv_blocks, *dctx_blocks, *stats_blocks, own_bias)


def project_out(x, context, w_out):
    rows, width = x.shape
    step = 256

    def body(x_ref, ctx_ref, w_ref, out_ref):
        out_ref[...] = (
            x_ref[...].astype(jnp.float32) + nn_dot(ctx_ref[...], w_ref[...])
        ).astype(jnp.bfloat16)

    return pl.pallas_call(
        body,
        grid=(width // step,),
        in_specs=[
            pl.BlockSpec((rows, step), lambda n: (0, n)),
            pl.BlockSpec((rows, width), lambda n: (0, 0)),
            pl.BlockSpec((width, step), lambda n: (0, n)),
        ],
        out_specs=pl.BlockSpec((rows, step), lambda n: (0, n)),
        out_shape=jax.ShapeDtypeStruct((rows, width), jnp.bfloat16),
        compiler_params=params("arbitrary"),
        cost_estimate=pl.CostEstimate(
            flops=2 * rows * width * width, bytes_accessed=2 * width * width, transcendentals=0
        ),
        name="project_out",
    )(x, context, w_out)


def input_gradient(x, dy, gain, dq, dk, dv, w_qkv):
    rows, width = x.shape
    step = width // 2
    halves = width // step

    def body(x_ref, dy_ref, gain_ref, dq_ref, dk_ref, dv_ref, w_ref, out_ref, acc_ref):
        n = pl.program_id(0)

        @pl.when(n == 0)
        def _():
            acc_ref[...] = nt_dot(dq_ref[...], w_ref[...])

        @pl.when(jnp.logical_and(n > 0, n < halves))
        def _():
            acc_ref[...] += nt_dot(dq_ref[...], w_ref[...])

        @pl.when(jnp.logical_and(n >= halves, n < 2 * halves))
        def _():
            acc_ref[...] += nt_dot(dk_ref[...], w_ref[...])

        @pl.when(n >= 2 * halves)
        def _():
            acc_ref[...] += nt_dot(dv_ref[...], w_ref[...])

        @pl.when(n == 3 * halves - 1)
        def _():
            xf = x_ref[...].astype(jnp.float32)
            inv = lax.rsqrt(jnp.mean(xf * xf, axis=-1, keepdims=True) + eps)
            scaled = gain_ref[...] * acc_ref[...]
            along = jnp.mean(xf * scaled, axis=-1, keepdims=True)
            grad = dy_ref[...].astype(jnp.float32) + inv * scaled - xf * (inv * inv * inv) * along
            out_ref[...] = grad.astype(jnp.bfloat16)

    whole = pl.BlockSpec((rows, width), lambda n: (0, 0))

    def piece(first):
        return pl.BlockSpec(
            (rows, step), lambda n: (0, jnp.clip(n - first * halves, 0, halves - 1))
        )

    return pl.pallas_call(
        body,
        grid=(3 * halves,),
        in_specs=[
            whole,
            whole,
            pl.BlockSpec((1, width), lambda n: (0, 0)),
            piece(0),
            piece(1),
            piece(2),
            pl.BlockSpec((width, step), lambda n: (0, n)),
        ],
        out_specs=whole,
        out_shape=jax.ShapeDtypeStruct((rows, width), jnp.bfloat16),
        scratch_shapes=[pltpu.VMEM((rows, width), jnp.float32)],
        compiler_params=params("arbitrary"),
        cost_estimate=pl.CostEstimate(
            flops=6 * rows * width * width, bytes_accessed=6 * width * width, transcendentals=0
        ),
        name="input_gradient",
    )(x, dy, gain, dq, dk, dv, w_qkv)


def shards(names, patches, cotangent, counts, gain, w_qkv, w_out):
    home, width = patches.shape
    members = lax.axis_size("k")
    devices = lax.axis_size(names)
    cap = 2 * home // devices
    outer = lax.axis_size("o")
    inner = lax.axis_size("j")
    own = lax.axis_index(names)
    group = lax.axis_index("o") * inner + lax.axis_index("j")
    member = lax.axis_index("k")
    gain_row = gain.reshape(1, width)

    plan = counts.reshape(devices, devices)
    plan_row = lax.dynamic_index_in_dim(plan, own, 0, keepdims=False)
    order = jnp.arange(devices, dtype=jnp.int32)
    offsets = jnp.sum(jnp.where(order[None, :] < order[:, None], plan_row[None, :], 0), axis=1)
    slots = jnp.arange(cap, dtype=jnp.int32)
    row_of_slot = jnp.where(slots[None, :] < plan_row[:, None], offsets[:, None] + slots[None, :], -1)
    if names == ("o", "k", "j"):
        row_of_slot = row_of_slot.reshape(outer, inner, members, cap).transpose(0, 2, 1, 3)
    row_of_slot = row_of_slot.reshape(devices * cap)
    place = (
        row_of_slot[:, None] == jnp.arange(home, dtype=jnp.int32)[None, :]
    ).astype(jnp.bfloat16)

    def pack(values):
        return nn_dot(place, values).astype(jnp.bfloat16)

    def unpack(values):
        return lax.dot_general(
            place, values, (((0,), (0,)), ((), ())), preferred_element_type=jnp.float32
        ).astype(jnp.bfloat16)

    def route(values):
        shaped = values.reshape(devices, cap, width)
        moved = lax.all_to_all(shaped, names, split_axis=0, concat_axis=0, tiled=True)
        return moved.reshape(devices * cap, width)

    def swap(values, bits):
        pairs = [(m, m ^ bits) for m in range(members)]
        return lax.ppermute(values, "k", pairs)

    def collect(values):
        held = {0: values}
        bit = members // 2
        while bit:
            for place_held in sorted(held, reverse=True):
                held[place_held ^ bit] = swap(held[place_held], bit)
            bit //= 2
        return [held[b] for b in range(members)]

    x = route(pack(patches))
    dy = route(pack(cotangent))
    x_blocks = collect(x)
    dy_blocks = collect(dy)

    incoming = lax.dynamic_index_in_dim(
        counts.reshape(devices, outer * inner, members), group, 1, keepdims=False
    )
    partner = jnp.arange(members, dtype=jnp.int32) ^ member
    arrivals = jnp.take(incoming, partner, axis=1).T
    live = slots[None, None, :] < arrivals[:, :, None]
    bias = jnp.where(live, 0.0, DEAD).reshape(members, devices * cap)

    qkv_blocks = [norm_project(block, gain_row, w_qkv) for block in x_blocks]
    dctx_blocks = [back_project(block, w_out) for block in dy_blocks]
    context, dq, stats = query_side(qkv_blocks, dctx_blocks[0], bias.reshape(1, -1))
    output = project_out(x, context, w_out)
    back_out = route(output)
    stats_blocks = [stats] + [swap(stats, b) for b in range(1, members)]
    dk, dv = key_side(qkv_blocks, dctx_blocks, stats_blocks, bias[0].reshape(-1, 1))
    grad = input_gradient(x, dy, gain_row, dq, dk, dv, w_qkv)
    back_grad = route(grad)
    return unpack(back_out), unpack(back_grad)


def solution(mesh):
    dp = mesh.shape["dp"]
    enc = mesh.shape["enc"]
    if dp % enc == 0:
        names, sizes = ("o", "k", "j"), (dp // enc, enc, enc)
    else:
        names, sizes = ("o", "j", "k"), (dp, 1, enc)
    fine = Mesh(mesh.devices.reshape(sizes), names)
    return jax.shard_map(
        functools.partial(shards, names),
        mesh=fine,
        in_specs=(P(names, None), P(names, None), P(), P(), P(), P()),
        out_specs=(P(names, None), P(names, None)),
        check_vma=False,
    )
```
